256 devices in a mesh: dp: 16 (over z, core), seq: 16 (over y, x).
Axes of the slice: x: 4, y: 4, z: 8, core: 2. Of those that a mesh axis runs over, the one named last changes fastest.
Arguments:
- layer_in: bfloat16 [16, 2048, 2560], P('dp', 'seq'), may hold values from -6 to 6
- scan_in: bfloat16 [16, 2048, 2560], P('dp', 'seq'), may hold values from -6 to 6
- step_size: float32 [16, 2048, 40], P('dp', 'seq'), may hold values from 0.0024 to 0.041
- b_weight: bfloat16 [2560, 64], replicated, may hold values from -0.125 to 0.125
- c_weight: bfloat16 [2560, 64], replicated, may hold values from -0.125 to 0.125
- decay_rate: float32 [40], replicated, may hold values from 0.0005 to 10
- skip_gain: float32 [40], replicated, may hold values from 0.25 to 1.75
- out_grad: bfloat16 [16, 2048, 2560], P('dp', 'seq'), may hold values from -6 to 6
- doc_lengths: int32 [16, 4], P('dp'), may hold values from 1 to 1024, 2048 in all within a row
- block_order: int32 [16, 16], P('dp'), may hold values from 0 to 15, each once within a row
Outputs:
- scan_out: bfloat16 [16, 2048, 2560], P('dp', 'seq')
- b_weight_grad: float32 [2560, 64], replicated
- c_weight_grad: float32 [2560, 64], replicated
The draws below stay inside these ranges and needn't reach their ends.
Inputs may be any that keep to these rules, and one draw needn't show every extreme that they name: `block_order`: each row holds 0 to 15 once each. `doc_lengths`: each row sums to 2048; its longest document has 1024 tokens.
All inputs are finite; a program needn't handle non-finite values.
Results may differ from the reference program's by a relative error of at most 0.0055.
Values sent between devices are 32-bit elements.
No kernel may reach another device: no remote copies, remote signals or barrier semaphores. Data moves between devices by JAX's collectives and lax.ppermute only.
A program may use at most 128 MiB of HBM per device.

```python
import math
import jax
import jax.numpy as jnp
import numpy as np
from jax import lax

D = 2560
INNER = 2560
STATE = 64
HEAD_DIM = 64
HEADS = 40
T_DEV = 128
DOCS = 4
SEQLEN = 2048
MOSTLEN = 1024
GROUPS = 16
N_SEQ = 16


def draw_step_size(key, part):
    key = jax.random.fold_in(key, 11)
    jitter_key, level_key = jax.random.split(key)
    jitter = jax.random.uniform(jitter_key, (GROUPS, SEQLEN // T_DEV, T_DEV, HEADS), jnp.float32, -0.7, 0.7)
    block_level = jax.random.uniform(level_key, (GROUPS, SEQLEN // T_DEV, 1, HEADS), jnp.float32, -0.7, 0.7)
    return (0.01 * jnp.exp(jitter + block_level)).reshape(GROUPS, SEQLEN, HEADS)


def draw_decay_rate(key, part):
    key = jax.random.fold_in(key, 23)
    pick_key, slow_key, fast_key = jax.random.split(key, 3)
    slow_share = 0.5
    slow_mask = jax.random.uniform(pick_key, (HEADS,), jnp.float32) < slow_share
    slow_rate = jnp.exp(jax.random.uniform(slow_key, (HEADS,), jnp.float32, math.log(0.0005), math.log(0.005)))
    fast_rate = jnp.exp(jax.random.uniform(fast_key, (HEADS,), jnp.float32, math.log(2.0), math.log(10.0)))
    return jnp.where(slow_mask, slow_rate, fast_rate)


def shard_levels(own_key, shape, pieces, smallest, high):
    def one(position, shards_of):
        draws = jax.random.uniform(jax.random.fold_in(jax.random.fold_in(own_key, 6), position), (shards_of,), jnp.float32, smallest / len(pieces), high / len(pieces))
        return jnp.repeat(jnp.exp(draws), shape[position] // shards_of).reshape((-1,) + (1,) * (len(shape) - position - 1))

    gain = one(*pieces[0])
    for cut in pieces[1:]:
        gain = gain * one(*cut)
    return gain


def split_up(number_of, total, reach, lean):
    portions = [(1 << 20) // math.isqrt(grade ** lean) + 1 for grade in range(2, number_of + 1)]
    spare, counts = total - reach - (number_of - 1), [1] * (number_of - 1)
    while spare > 0:
        free = [i for i in range(number_of - 1) if counts[i] < reach]
        whole, budget = sum([portions[i] for i in free]), spare
        for i in free:
            more = min(reach - counts[i], max(1, budget * portions[i] // whole), spare)
            counts[i] = counts[i] + more
            spare = spare - more
    return np.array([reach] + counts)


def ragged_sizes(rng, count, total, most, slope):
    if count == 2:
        one = jax.random.randint(rng, (), max(1, total - most), min(most, total - 1) + 1)
        return jnp.stack([one, total - one])
    tallies = jnp.asarray(split_up(count, total, most, slope), jnp.int32)
    couples = (count - 1) // 2
    donor, receiver = tallies[1:1 + 2 * couples:2], tallies[2:2 + 2 * couples:2]
    slack = jnp.minimum(donor - 1, most - receiver)
    shifted = jax.random.randint(jax.random.fold_in(rng, 1), (couples,), 0, 1 << 20) % (slack + 1)
    tallies = tallies.at[1:1 + 2 * couples:2].set(donor - shifted).at[2:2 + 2 * couples:2].set(receiver + shifted)
    return tallies[jax.random.permutation(jax.random.fold_in(rng, 2), count)]


def normal_values(key, extent, scale, reach, cuts=(), kind=jnp.bfloat16):
    level = shard_levels(key, extent, cuts, -0.22, 0.18) if cuts else 1.0
    values = jax.random.normal(key, extent, jnp.float32) * scale * level
    return jnp.minimum(jnp.maximum(values, -reach), reach).astype(kind)


def setup_inputs(seed: int = 0) -> dict:
    arg_keys = jax.random.split(jax.random.key(seed), 11)
    return {
        "layer_in": normal_values(arg_keys[0], (GROUPS, SEQLEN, D), 1.0, 6.0, ((0, 16), (1, 16))),
        "scan_in": normal_values(arg_keys[1], (GROUPS, SEQLEN, INNER), 1.0, 6.0, ((0, 16), (1, 16))),
        "step_size": draw_step_size(jax.random.fold_in(arg_keys[10], 71), 0),
        "b_weight": normal_values(arg_keys[3], (D, STATE), D ** -0.5, 0.125),
        "c_weight": normal_values(arg_keys[4], (D, STATE), D ** -0.5, 0.125),
        "decay_rate": draw_decay_rate(jax.random.fold_in(arg_keys[10], 71), 0),
        "skip_gain": jnp.clip(1.0 + 0.15 * jax.random.normal(arg_keys[6], (HEADS,), jnp.float32), 0.25, 1.75),
        "out_grad": normal_values(arg_keys[7], (GROUPS, SEQLEN, INNER), 1.0, 6.0, ((0, 16), (1, 16))),
        "doc_lengths": jax.vmap(lambda own: ragged_sizes(own, DOCS, SEQLEN, MOSTLEN, 2))(jax.random.split(arg_keys[8], GROUPS)).reshape((GROUPS, DOCS)).astype(jnp.int32),
        "block_order": jax.vmap(lambda own: jax.random.permutation(own, N_SEQ))(jax.random.split(arg_keys[9], GROUPS)).reshape((GROUPS, N_SEQ)).astype(jnp.int32),
    }


def group_pass(scan_grp, step_grp, grad_grp, lengths, order_row, b_grp, c_grp, decay_rate, skip_gain):
    head_count = decay_rate.shape[0]
    inverse = jnp.zeros((N_SEQ,), jnp.int32).at[order_row].set(jnp.arange(N_SEQ, dtype=jnp.int32))

    def to_sequence(values):
        return values.reshape((N_SEQ, T_DEV) + values.shape[1:])[inverse].reshape((SEQLEN,) + values.shape[1:])

    def to_held(values):
        return values.reshape((N_SEQ, T_DEV) + values.shape[1:])[order_row].reshape((SEQLEN,) + values.shape[1:])

    seq_x = to_sequence(scan_grp).reshape(SEQLEN, head_count, HEAD_DIM)
    seq_grad = to_sequence(grad_grp).reshape(SEQLEN, head_count, HEAD_DIM)
    seq_step = to_sequence(step_grp)
    seq_b = to_sequence(b_grp).astype(jnp.float32)
    seq_c = to_sequence(c_grp).astype(jnp.float32)
    doc_ends = jnp.cumsum(lengths, dtype=jnp.int32)
    doc_starts = doc_ends - lengths
    positions = jnp.arange(SEQLEN, dtype=jnp.int32)
    begins = jnp.any(positions[:, None] == doc_starts[None, :], axis=1)
    decay = jnp.where(begins[:, None], jnp.float32(0.0), jnp.exp(-seq_step * decay_rate[None, :]))

    def forward(state_now, inputs):
        decay_now, step_now, x_row, b_row, c_row, grad_row = inputs
        x_float = x_row.astype(jnp.float32)
        state_now = decay_now[:, None, None] * state_now + (step_now[:, None] * x_float)[:, :, None] * b_row[None, None, :]
        out_row = jnp.sum(state_now * c_row[None, None, :], axis=2) + skip_gain[:, None] * x_float
        dc_row = jnp.sum(state_now * grad_row.astype(jnp.float32)[:, :, None], axis=(0, 1))
        return state_now, (out_row.astype(jnp.bfloat16), dc_row.astype(jnp.bfloat16))

    zero_state = jnp.zeros((head_count, HEAD_DIM, STATE), jnp.float32)
    _, (outs_seq, dc_seq) = lax.scan(forward, zero_state, (decay, seq_step, seq_x, seq_b, seq_c, seq_grad))
    next_decay = jnp.concatenate([decay[1:], jnp.zeros((1, head_count), jnp.float32)], axis=0)

    def backward(adjoint, inputs):
        decay_next, step_now, x_row, c_row, grad_row = inputs
        adjoint = decay_next[:, None, None] * adjoint + grad_row.astype(jnp.float32)[:, :, None] * c_row[None, None, :]
        db_row = jnp.sum(adjoint * (step_now[:, None] * x_row.astype(jnp.float32))[:, :, None], axis=(0, 1))
        return adjoint, db_row.astype(jnp.bfloat16)

    _, db_seq = lax.scan(backward, zero_state, (next_decay, seq_step, seq_x, seq_c, seq_grad), reverse=True)
    return to_held(outs_seq.reshape(SEQLEN, head_count * HEAD_DIM)), to_held(dc_seq), to_held(db_seq)


def reference(layer_in, scan_in, step_size, b_weight, c_weight, decay_rate, skip_gain, out_grad, doc_lengths, block_order):
    group_count = layer_in.shape[0]
    token_rows = layer_in.reshape(-1, D)
    b_all = jnp.dot(token_rows, b_weight, preferred_element_type=jnp.float32).astype(jnp.bfloat16).reshape(group_count, SEQLEN, STATE)
    c_all = jnp.dot(token_rows, c_weight, preferred_element_type=jnp.float32).astype(jnp.bfloat16).reshape(group_count, SEQLEN, STATE)

    def run_group(inputs):
        return group_pass(*inputs, decay_rate, skip_gain)

    outs_all, dc_all, db_all = lax.map(run_group, (scan_in, step_size, out_grad, doc_lengths, block_order, b_all, c_all))
    scale = 1.0 / (group_count * SEQLEN)
    b_grad = jnp.dot(token_rows.T, db_all.reshape(-1, STATE), preferred_element_type=jnp.float32) * scale
    c_grad = jnp.dot(token_rows.T, dc_all.reshape(-1, STATE), preferred_element_type=jnp.float32) * scale
    return outs_all, b_grad, c_grad
```

```python
import functools

import jax
import jax.numpy as jnp
from jax import lax
from jax.experimental import pallas as pl
from jax.experimental.pallas import tpu as pltpu
from jax.sharding import Mesh
from jax.sharding import PartitionSpec as P

SEQ = ("y", "x")
DP = ("z", "core")
F32 = jnp.float32
BF16 = jnp.bfloat16
CHUNK = 256
EXTRA = 128

VMEM = pl.BlockSpec(memory_space=pltpu.VMEM)
HBM = pl.BlockSpec(memory_space=pltpu.HBM)
SMEM = pl.BlockSpec(memory_space=pltpu.SMEM)
ALL_VMEM = pltpu.CompilerParams(vmem_limit_bytes=67043328)
PARAMS = pltpu.CompilerParams(vmem_limit_bytes=48 * 1024 * 1024)


def dot(a, b, dims=((1,), (0,))):
    return lax.dot_general(a, b, (dims, ((), ())), preferred_element_type=F32)


def dot_nt(a, b):
    return dot(a, b, ((1,), (1,)))


def dot_tn(a, b):
    return dot(a, b, ((0,), (0,)))


def slot_index():
    return lax.axis_index("y") * lax.axis_size("x") + lax.axis_index("x")


def spread(values, first, count, width):
    rows = values.shape[0]
    per = 128 // width
    lane = lax.broadcasted_iota(jnp.int32, (rows, 128), 1)
    parts = []
    for j in range(0, count, per):
        piece = jnp.broadcast_to(values[:, first + j : first + j + 1], (rows, 128))
        for k in range(1, per):
            other = jnp.broadcast_to(values[:, first + j + k : first + j + k + 1], (rows, 128))
            piece = jnp.where(lane >= k * width, other, piece)
        parts.append(piece)
    return jnp.concatenate(parts, axis=1) if len(parts) > 1 else parts[0]


def count_started(starts, position):
    return sum((start <= position).astype(jnp.int32) for start in starts)


def states_kernel(
    lengths_hbm, order_hbm, layer_hbm, x_hbm, grad_hbm, step_hbm, bw_hbm, cw_hbm, rate_hbm, gain_hbm,
    send_ref, layer_ref, x_ref, pushed_ref, seen_ref, b_ref, c_ref, c_linked_ref, scores_ref,
    causal_ref, linked_ref, last_ref, enter_ref, total_ref, gain_ref,
    lengths_ref, order_ref, grad_ref, step_ref, bw_ref, cw_ref, rate_ref, sems,
):
    pairs = (
        (lengths_hbm, lengths_ref), (order_hbm, order_ref), (rate_hbm, rate_ref),
        (step_hbm, step_ref), (bw_hbm, bw_ref), (cw_hbm, cw_ref), (layer_hbm, layer_ref),
        (x_hbm, x_ref), (grad_hbm, grad_ref), (gain_hbm, gain_ref),
    )
    copies = [pltpu.make_async_copy(a, b, sems.at[i]) for i, (a, b) in enumerate(pairs)]
    for copy in copies:
        copy.start()
    rows, inner = x_ref.shape[1:]
    heads = rate_ref.shape[1]
    width = inner // heads
    docs = lengths_ref.shape[1]
    blocks = send_ref.shape[0]
    half = blocks // 2
    state = bw_ref.shape[0]
    for copy in copies[:4]:
        copy.wait()
    first = order_ref[0, slot_index()] * rows
    starts = [jnp.int32(0)]
    for j in range(docs - 1):
        starts.append(starts[-1] + lengths_ref[0, j])
    across = (rows, rows)
    at_row = lax.broadcasted_iota(jnp.int32, across, 0)
    at_column = lax.broadcasted_iota(jnp.int32, across, 1)
    column = count_started(starts, first + at_row)
    row = count_started(starts, first + at_column)
    before = count_started(starts, first - 1)
    last = count_started(starts, first + rows - 1)
    tri = at_row >= at_column
    causal = tri & (column == row)
    linked = column[:, :state] == before
    in_last = column[:, :state] == last
    causal_ref[...] = causal.astype(F32)
    linked_ref[...] = linked.astype(F32)
    last_ref[...] = in_last.astype(F32)
    steps = step_ref[0].T
    logs = -(steps * rate_ref[...])
    cum = lax.dot_general(
        tri.astype(F32), logs, (((1,), (0,)), ((), ())),
        precision=lax.Precision.HIGHEST, preferred_element_type=F32,
    )
    enter = jnp.exp(cum)
    leave = steps * jnp.exp(-cum)
    enter_ref[...] = enter
    whole = enter[rows - 1 :, :]
    total_ref[...] = whole
    total = whole * (before == last).astype(F32)
    send_ref[:, :, inner : inner + heads] = jnp.broadcast_to(total[None], (blocks, 8, heads))
    for copy in copies[4:7]:
        copy.wait()
    tokens = layer_ref[0]
    b_mat = dot_nt(tokens, bw_ref[...]).astype(BF16)
    c_mat = dot_nt(tokens, cw_ref[...]).astype(BF16)
    b_ref[...] = b_mat
    c_ref[...] = c_mat
    scores_ref[...] = jnp.where(causal, dot_nt(c_mat, b_mat), 0.0).astype(BF16)
    b_last = jnp.where(in_last, b_mat.astype(F32), 0.0).astype(BF16)
    c_linked = jnp.where(linked, c_mat.astype(F32), 0.0).astype(BF16)
    c_linked_ref[...] = c_linked
    for copy in copies[7:]:
        copy.wait()
    per = CHUNK // width
    for at in range(0, inner, CHUNK):
        cols = slice(at, at + CHUNK)
        h = at // width
        pushed = (spread(leave, h, per, width) * x_ref[0, :, cols].astype(F32)).astype(BF16)
        seen = (spread(enter, h, per, width) * grad_ref[0, :, cols].astype(F32)).astype(BF16)
        pushed_ref[:, cols] = pushed
        seen_ref[:, cols] = seen
        own = dot_tn(b_last, pushed) * spread(whole, h, per, width)
        adj = dot_tn(c_linked, seen)
        send_ref[:half, :, cols] = own.reshape(half, 8, CHUNK)
        send_ref[half:, :, cols] = adj.reshape(half, 8, CHUNK)


def chain_kernel(order_ref, got_ref, out_ref, held_ref):
    blocks, _, inner = out_ref.shape
    heads = inner // 64
    for slot in range(blocks):
        held_ref[order_ref[0, slot]] = jnp.int32(slot)
    backward = slot_index() >= blocks // 2
    carry = jnp.zeros(out_ref.shape[1:], F32)
    for k in range(blocks):
        slot = held_ref[jnp.where(backward, blocks - 1 - k, k)]
        out_ref[slot] = carry
        if k < blocks - 1:
            totals = got_ref[slot, :, inner : inner + heads]
            carry = carry * spread(totals, 0, heads, 64) + got_ref[slot, :, :inner]


def grads_kernel(
    layer_ref, got_ref, pushed_ref, seen_ref, b_ref, c_ref, causal_ref, linked_ref, last_ref,
    total_ref,
    came_ref, keep_ref, give_ref, ret_ref,
):
    rows, inner = pushed_ref.shape
    heads = total_ref.shape[1]
    width = inner // heads
    blocks = got_ref.shape[0]
    half = blocks // 2
    state = b_ref.shape[1]
    whole = total_ref[...]
    per = CHUNK // width
    for at in range(0, inner, CHUNK):
        cols = slice(at, at + CHUNK)
        back = got_ref[half:, :, cols].reshape(state, CHUNK)
        came_ref[:, cols] = got_ref[:half, :, cols].reshape(state, CHUNK).astype(BF16)
        ret_ref[:, cols] = (back * spread(whole, at // width, per, width)).astype(BF16)
    pushed = pushed_ref[...]
    seen = seen_ref[...]
    mixing = jnp.where(causal_ref[...] > 0.5, dot_nt(seen, pushed), 0.0).astype(BF16)
    linked = linked_ref[...] > 0.5
    in_last = last_ref[...] > 0.5
    d_c = dot(mixing, b_ref[...]) + jnp.where(linked, dot_nt(seen, came_ref[...]), 0.0)
    d_b = dot_tn(mixing, c_ref[...]) + jnp.where(in_last, dot_nt(pushed, ret_ref[...]), 0.0)
    scale = 1.0 / (rows * blocks * lax.axis_size("z") * lax.axis_size("core"))
    first = lax.axis_index("core") == 0
    mine = jnp.where(first, d_b, d_c).astype(BF16)
    other = jnp.where(first, d_c, d_b).astype(BF16)
    columns = layer_ref.shape[2] // 128
    for at in range(0, layer_ref.shape[2], CHUNK):
        tokens = layer_ref[0, :, at : at + CHUNK]
        for side, to_ref in ((other, give_ref), (mine, keep_ref)):
            part = dot_tn(side, tokens) * scale
            for r in range(state // 8):
                for c in range(CHUNK // 128):
                    tile = r * columns + at // 128 + c
                    to_ref[tile] = part[8 * r : 8 * r + 8, 128 * c : 128 * c + 128]


def output_kernel(x_ref, gain_ref, came_ref, pushed_ref, scores_ref, c_linked_ref, enter_ref, out_ref):
    _, inner = pushed_ref.shape
    heads = gain_ref.shape[1]
    width = inner // heads
    scores = scores_ref[...]
    c_linked = c_linked_ref[...]
    enter = enter_ref[...]
    gain = gain_ref[...]
    per = CHUNK // width
    for at in range(0, inner, CHUNK):
        cols = slice(at, at + CHUNK)
        h = at // width
        mixed = dot(scores, pushed_ref[:, cols]) + dot(c_linked, came_ref[:, cols])
        skip = spread(gain, h, per, width) * x_ref[0, :, cols].astype(F32)
        out_ref[0, :, cols] = (spread(enter, h, per, width) * mixed + skip).astype(BF16)


def unpack_kernel(mine_ref, other_ref, b_ref, c_ref):
    columns = b_ref.shape[1] // 128

    def write(from_ref, to_ref):
        for r in range(to_ref.shape[0] // 8):
            for c in range(columns):
                to_ref[8 * r : 8 * r + 8, 128 * c : 128 * c + 128] = from_ref[r * columns + c]

    first = lax.axis_index("core") == 0

    @pl.when(first)
    def _():
        write(mine_ref, b_ref)
        write(other_ref, c_ref)

    @pl.when(jnp.logical_not(first))
    def _():
        write(other_ref, b_ref)
        write(mine_ref, c_ref)


def shape(*dims, dtype=F32):
    return jax.ShapeDtypeStruct(dims, dtype)


def swap_cores(a):
    return lax.ppermute(a, "core", [(0, 1), (1, 0)])


def exchange(a, axes):
    return lax.all_to_all(a, axes, 0, 0, tiled=True)


def everywhere(a, axes):
    return exchange(jnp.broadcast_to(a[None], (lax.axis_size(axes),) + a.shape), axes)


def per_device(
    layer_in, scan_in, step_size, b_weight, c_weight, decay_rate, skip_gain, out_grad, doc_lengths,
    block_order,
):
    _, rows, inner = scan_in.shape
    width_in, state = b_weight.shape
    tile_cols = width_in // 128
    heads = decay_rate.shape[0]
    blocks = lax.axis_size(SEQ)
    docs = doc_lengths.shape[1]
    states = pl.pallas_call(
        states_kernel,
        out_shape=(
            shape(blocks, 8, inner + EXTRA),
            shape(1, rows, width_in, dtype=BF16),
            shape(1, rows, inner, dtype=BF16),
            shape(rows, inner, dtype=BF16),
            shape(rows, inner, dtype=BF16),
            shape(rows, state, dtype=BF16),
            shape(rows, state, dtype=BF16),
            shape(rows, state, dtype=BF16),
            shape(rows, rows, dtype=BF16),
            shape(rows, rows),
            shape(rows, state),
            shape(rows, state),
            shape(rows, heads),
            shape(1, heads),
            shape(1, heads),
        ),
        in_specs=[HBM] * 10,
        out_specs=(VMEM,) * 15,
        scratch_shapes=[
            pltpu.SMEM((1, docs), jnp.int32),
            pltpu.SMEM((1, blocks), jnp.int32),
            pltpu.VMEM((1, rows, inner), BF16),
            pltpu.VMEM((1, heads, rows), F32),
            pltpu.VMEM((state, width_in), BF16),
            pltpu.VMEM((state, width_in), BF16),
            pltpu.VMEM((1, heads), F32),
            pltpu.SemaphoreType.DMA((10,)),
        ],
        compiler_params=ALL_VMEM,
    )(
        doc_lengths, block_order, layer_in, scan_in, out_grad, jnp.swapaxes(step_size, 1, 2),
        b_weight.T, c_weight.T, decay_rate[None], skip_gain[None],
    )
    send, layer, x, pushed, seen, b_mat, c_mat, c_linked, scores, causal, linked, in_last = states[:12]
    enter, total, gain = states[12:]
    got = exchange(send, SEQ)
    carried = pl.pallas_call(
        chain_kernel,
        out_shape=shape(blocks, 8, inner),
        in_specs=[SMEM, VMEM],
        out_specs=VMEM,
        scratch_shapes=[pltpu.SMEM((blocks,), jnp.int32)],
        compiler_params=PARAMS,
    )(block_order, got)
    back = exchange(carried, SEQ)
    came, keep, give = pl.pallas_call(
        grads_kernel,
        out_shape=(
            shape(state, inner, dtype=BF16),
            shape(state // 8 * tile_cols, 8, 128),
            shape(state // 8 * tile_cols, 8, 128),
        ),
        in_specs=[VMEM] * 10,
        out_specs=(VMEM,) * 3,
        scratch_shapes=[pltpu.VMEM((state, inner), BF16)],
        compiler_params=PARAMS,
        cost_estimate=pl.CostEstimate(flops=10**9, bytes_accessed=10**6, transcendentals=0),
    )(layer, back, pushed, seen, b_mat, c_mat, causal, linked, in_last, total)
    scan_out = pl.pallas_call(
        output_kernel,
        out_shape=shape(1, rows, inner, dtype=BF16),
        in_specs=[VMEM] * 7,
        out_specs=VMEM,
        compiler_params=PARAMS,
        cost_estimate=pl.CostEstimate(flops=10**9, bytes_accessed=10**6, transcendentals=0),
    )(x, gain, came, pushed, scores, c_linked, enter)
    local = keep + swap_cores(give)
    tiles = local.shape[0] // blocks
    share = jnp.sum(exchange(local.reshape(blocks, tiles, 8, 128), SEQ), axis=0)
    share = jnp.sum(everywhere(share, "z"), axis=0)
    mine = everywhere(share, SEQ).reshape(local.shape)
    other = swap_cores(mine)
    b_grad, c_grad = pl.pallas_call(
        unpack_kernel,
        out_shape=(shape(state, width_in), shape(state, width_in)),
        in_specs=[VMEM] * 2,
        out_specs=(VMEM,) * 2,
        compiler_params=PARAMS,
    )(mine, other)
    return scan_out, b_grad.T, c_grad.T


def solution(mesh):
    seq = mesh.shape["seq"]
    side = 4 if seq % 4 == 0 else 1
    split = Mesh(
        mesh.devices.reshape(mesh.shape["dp"] // 2, 2, seq // side, side), ("z", "core", "y", "x")
    )
    rows = P(DP, SEQ, None)
    group = P(DP, None)
    in_specs = (rows, rows, rows, P(), P(), P(), P(), rows, group, group)
    return jax.shard_map(
        per_device, mesh=split, in_specs=in_specs, out_specs=(rows, P(), P()), check_vma=False
    )
```

```python
import jax
import jax.numpy as jnp
from jax import lax
from jax.experimental import pallas as pl
from jax.experimental.pallas import tpu as pltpu
from jax.sharding import Mesh
from jax.sharding import PartitionSpec as P


SEQ = ("y", "x")
DP = ("z", "core")
F32 = jnp.float32
BF16 = jnp.bfloat16
CHUNK = 256
EXTRA = 128
OUT = 512


VMEM = pl.BlockSpec(memory_space=pltpu.VMEM)
HBM = pl.BlockSpec(memory_space=pltpu.HBM)
SMEM = pl.BlockSpec(memory_space=pltpu.SMEM)
ALL_VMEM = pltpu.CompilerParams(vmem_limit_bytes=67043328)
PARAMS = pltpu.CompilerParams(vmem_limit_bytes=48 * 1024 * 1024)


def dot(a, b, dims=((1,), (0,))):
    return lax.dot_general(a, b, (dims, ((), ())), preferred_element_type=F32)


def dot_nt(a, b):
    return dot(a, b, ((1,), (1,)))


def dot_tn(a, b):
    return dot(a, b, ((0,), (0,)))


def slot_index():
    return lax.axis_index("y") * lax.axis_size("x") + lax.axis_index("x")


def spread(values, first, count, width):
    rows = max(values.shape[0], 8)
    table = jnp.broadcast_to(values, (rows, 128))
    lane = lax.broadcasted_iota(jnp.int32, (rows, 128), 1) // width
    per = 128 // width
    parts = [
        jnp.take_along_axis(table, lane + (first + j), axis=1, mode="promise_in_bounds")
        for j in range(0, count, per)
    ]
    whole = jnp.concatenate(parts, axis=1) if len(parts) > 1 else parts[0]
    return whole[: values.shape[0]]


def count_started(starts, position):
    return sum((start <= position).astype(jnp.int32) for start in starts)


def states_kernel(
    lengths_hbm, order_hbm, layer_hbm, x_hbm, grad_hbm, step_hbm, bw_hbm, cw_hbm, rate_hbm,
    send_hbm, pushed_hbm, seen_hbm, mats_hbm, scores_hbm, enter_hbm,
    lengths_ref, order_ref, layer_ref, x_ref, grad_ref, step_ref, weights_ref, rate_ref,
    send_ref, pushed_ref, seen_ref, mats_ref, scores_ref, enter_ref, in_sems, out_sems,
):
    state = bw_hbm.shape[0]
    pairs = (
        (lengths_hbm, lengths_ref), (order_hbm, order_ref), (rate_hbm, rate_ref),
        (step_hbm, step_ref), (layer_hbm, layer_ref), (bw_hbm, weights_ref.at[:state]),
        (cw_hbm, weights_ref.at[state:]),
        (x_hbm, x_ref), (grad_hbm, grad_ref),
    )
    copies = [pltpu.make_async_copy(a, b, in_sems.at[i]) for i, (a, b) in enumerate(pairs)]
    for copy in copies:
        copy.start()
    leaving = []

    def leave_for(from_ref, to_ref):
        copy = pltpu.make_async_copy(from_ref, to_ref, out_sems.at[len(leaving)])
        copy.start()
        leaving.append(copy)

    rows, inner = x_ref.shape[1:]
    heads = rate_ref.shape[1]
    width = inner // heads
    docs = lengths_ref.shape[1]
    blocks = send_ref.shape[0]
    half = blocks // 2
    for copy in copies[:4]:
        copy.wait()
    first = order_ref[0, slot_index()] * rows
    starts = [jnp.int32(0)]
    for j in range(docs - 1):
        starts.append(starts[-1] + lengths_ref[0, j])
    across = (rows, rows)
    at_row = lax.broadcasted_iota(jnp.int32, across, 0)
    at_column = lax.broadcasted_iota(jnp.int32, across, 1)
    column = count_started(starts, first + at_row)
    row = count_started(starts, first + at_column)
    before = count_started(starts, first - 1)
    last = count_started(starts, first + rows - 1)
    tri = at_row >= at_column
    causal = tri & (column == row)
    linked = column[:, :state] == before
    in_last = column[:, :state] == last
    logs_up = -(step_ref[0] * rate_ref[...].T)
    spare = jnp.zeros((128 - heads, rows), F32)
    cum = lax.dot_general(
        tri.astype(F32), jnp.concatenate([logs_up, spare], axis=0), (((1,), (1,)), ((), ())),
        precision=lax.Precision.HIGHEST, preferred_element_type=F32,
    )
    steps = jnp.concatenate([step_ref[0], spare], axis=0).T
    enter = jnp.exp(cum)
    leave = steps * jnp.exp(-cum)
    enter_ref[...] = enter
    whole = enter[rows - 1 :, :]
    total = whole * (before == last).astype(F32)
    send_ref[:, :, inner:] = jnp.broadcast_to(total[None], (blocks, 8, 128))
    for copy in copies[4:7]:
        copy.wait()
    mats = dot_nt(layer_ref[0], weights_ref[...]).astype(BF16)
    b_mat = mats[:, :state]
    c_mat = mats[:, state:]
    scores_ref[0] = jnp.where(causal, dot_nt(c_mat, b_mat), 0.0).astype(BF16)
    scores_ref[1] = causal.astype(F32).astype(BF16)
    b_last = jnp.where(in_last, b_mat.astype(F32), 0.0).astype(BF16)
    c_linked = jnp.where(linked, c_mat.astype(F32), 0.0).astype(BF16)
    mats_ref[0] = b_mat
    mats_ref[1] = c_mat
    mats_ref[2] = c_linked
    mats_ref[3] = linked.astype(F32).astype(BF16)
    mats_ref[4] = in_last.astype(F32).astype(BF16)
    for copy in copies[7:]:
        copy.wait()
    per = CHUNK // width
    for at in range(0, inner, CHUNK):
        cols = slice(at, at + CHUNK)
        h = at // width
        pushed = (spread(leave, h, per, width) * x_ref[0, :, cols].astype(F32)).astype(BF16)
        seen = (spread(enter, h, per, width) * grad_ref[0, :, cols].astype(F32)).astype(BF16)
        pushed_ref[:, cols] = pushed
        seen_ref[:, cols] = seen
        own = dot_tn(b_last, pushed) * spread(whole, h, per, width)
        adj = dot_tn(c_linked, seen)
        send_ref[:half, :, cols] = own.reshape(half, 8, CHUNK)
        send_ref[half:, :, cols] = adj.reshape(half, 8, CHUNK)
        if (at + CHUNK) % OUT == 0:
            done = slice(at + CHUNK - OUT, at + CHUNK)
            leave_for(pushed_ref.at[:, done], pushed_hbm.at[:, done])
            leave_for(seen_ref.at[:, done], seen_hbm.at[:, done])
            end = at + CHUNK + (128 if at + CHUNK == inner else 0)
            done = slice(at + CHUNK - OUT, end)
            leave_for(send_ref.at[:, :, done], send_hbm.at[:, :, done])
        if at == 0:
            leave_for(mats_ref, mats_hbm)
            leave_for(scores_ref, scores_hbm)
            leave_for(enter_ref, enter_hbm)
    for copy in leaving:
        copy.wait()


def chain_kernel(order_ref, got_ref, out_ref, held_ref):
    blocks, _, inner = out_ref.shape
    heads = inner // 64
    for slot in range(blocks):
        held_ref[order_ref[0, slot]] = jnp.int32(slot)
    backward = slot_index() >= blocks // 2
    carry = jnp.zeros(out_ref.shape[1:], F32)
    for k in range(blocks):
        slot = held_ref[jnp.where(backward, blocks - 1 - k, k)]
        out_ref[slot] = carry
        if k < blocks - 1:
            totals = got_ref[slot, :, inner:]
            carry = carry * spread(totals, 0, heads, 64) + got_ref[slot, :, :inner]


def grads_kernel(
    layer_ref, got_ref, pushed_ref, seen_ref, mats_ref, scores_ref, enter_ref,
    came_ref, keep_ref, give_ref, ret_ref,
):
    rows, inner = pushed_ref.shape
    blocks = got_ref.shape[0]
    half = blocks // 2
    state = mats_ref.shape[2]
    whole = enter_ref[rows - 1 :, :]
    per = CHUNK // state
    for at in range(0, inner, CHUNK):
        cols = slice(at, at + CHUNK)
        back = got_ref[half:, :, cols].reshape(state, CHUNK)
        came_ref[:, cols] = got_ref[:half, :, cols].reshape(state, CHUNK).astype(BF16)
        ret_ref[:, cols] = (back * spread(whole, at // state, per, state)).astype(BF16)
    linked = mats_ref[3].astype(F32) > 0.5
    in_last = mats_ref[4].astype(F32) > 0.5
    pushed = pushed_ref[...]
    seen = seen_ref[...]
    causal = scores_ref[1].astype(F32) > 0.5
    mixing = jnp.where(causal, dot_nt(seen, pushed), 0.0).astype(BF16)
    d_b = dot_tn(mixing, mats_ref[1]) + jnp.where(in_last, dot_nt(pushed, ret_ref[...]), 0.0)
    d_c = dot(mixing, mats_ref[0]) + jnp.where(linked, dot_nt(seen, came_ref[...]), 0.0)
    scale = 1.0 / (rows * blocks * lax.axis_size("z") * lax.axis_size("core"))
    low = lax.axis_index("core") == 0
    mine = jnp.where(low, d_b, d_c).astype(BF16)
    other = jnp.where(low, d_c, d_b).astype(BF16)
    columns = layer_ref.shape[2] // 128
    for at in range(0, layer_ref.shape[2], CHUNK):
        tokens = layer_ref[0, :, at : at + CHUNK]
        for side, to_ref in ((other, give_ref), (mine, keep_ref)):
            part = dot_tn(side, tokens) * scale
            for r in range(state // 8):
                for c in range(CHUNK // 128):
                    tile = r * columns + at // 128 + c
                    to_ref[tile] = part[8 * r : 8 * r + 8, 128 * c : 128 * c + 128]


def output_kernel(x_ref, gain_ref, came_ref, pushed_ref, scores_ref, mats_ref, enter_ref, out_ref):
    inner = pushed_ref.shape[1]
    heads = gain_ref.shape[1]
    width = inner // heads
    scores = scores_ref[0]
    c_linked = mats_ref[2]
    enter = enter_ref[...]
    gain = jnp.concatenate([gain_ref[...].T, jnp.zeros((128 - heads, 1), F32)], axis=0).T
    per = CHUNK // width
    for at in range(0, inner, CHUNK):
        cols = slice(at, at + CHUNK)
        h = at // width
        mixed = dot(scores, pushed_ref[:, cols]) + dot(c_linked, came_ref[:, cols])
        skip = spread(gain, h, per, width) * x_ref[0, :, cols].astype(F32)
        out_ref[0, :, cols] = (spread(enter, h, per, width) * mixed + skip).astype(BF16)


def place(tiles_ref, whole_ref, b_hbm, c_hbm, to_b, sem):
    columns = whole_ref.shape[1] // 128
    for r in range(whole_ref.shape[0] // 8):
        for c in range(columns):
            whole_ref[8 * r : 8 * r + 8, 128 * c : 128 * c + 128] = tiles_ref[r * columns + c]

    @pl.when(to_b)
    def _():
        copy = pltpu.make_async_copy(whole_ref, b_hbm, sem)
        copy.start()
        copy.wait()

    @pl.when(jnp.logical_not(to_b))
    def _():
        copy = pltpu.make_async_copy(whole_ref, c_hbm, sem)
        copy.start()
        copy.wait()


def place_mine_kernel(tiles_ref, b_hbm, c_hbm, whole_ref, sem):
    place(tiles_ref, whole_ref, b_hbm, c_hbm, lax.axis_index("core") == 0, sem)


def place_other_kernel(tiles_ref, b_in, c_in, b_hbm, c_hbm, whole_ref, sem):
    place(tiles_ref, whole_ref, b_hbm, c_hbm, lax.axis_index("core") == 1, sem)


def shape(*dims, dtype=F32):
    return jax.ShapeDtypeStruct(dims, dtype)


def swap_cores(a):
    return lax.ppermute(a, "core", [(0, 1), (1, 0)])


def exchange(a, axes):
    return lax.all_to_all(a, axes, 0, 0, tiled=True)


def everywhere(a, axes):
    return exchange(jnp.broadcast_to(a[None], (lax.axis_size(axes),) + a.shape), axes)


def device_step(
    layer_in, scan_in, step_size, b_weight, c_weight, decay_rate, skip_gain, out_grad, doc_lengths,
    block_order,
):
    _, rows, inner = scan_in.shape
    width_in, state = b_weight.shape
    tile_cols = width_in // 128
    heads = decay_rate.shape[0]
    blocks = lax.axis_size(SEQ)
    docs = doc_lengths.shape[1]
    outs = (
        ((blocks, 8, inner + EXTRA), F32),
        ((rows, inner), BF16),
        ((rows, inner), BF16),
        ((5, rows, state), BF16),
        ((2, rows, rows), BF16),
        ((rows, 128), F32),
    )
    send, pushed, seen, mats, scores, enter = pl.pallas_call(
        states_kernel,
        out_shape=tuple(shape(*dims, dtype=dtype) for dims, dtype in outs),
        in_specs=[HBM] * 9,
        out_specs=(HBM,) * 6,
        scratch_shapes=[
            pltpu.SMEM((1, docs), jnp.int32),
            pltpu.SMEM((1, blocks), jnp.int32),
            pltpu.VMEM((1, rows, width_in), BF16),
            pltpu.VMEM((1, rows, inner), BF16),
            pltpu.VMEM((1, rows, inner), BF16),
            pltpu.VMEM((1, heads, rows), F32),
            pltpu.VMEM((2 * state, width_in), BF16),
            pltpu.VMEM((1, heads), F32),
            *[pltpu.VMEM(dims, dtype) for dims, dtype in outs],
            pltpu.SemaphoreType.DMA((9,)),
            pltpu.SemaphoreType.DMA((3 * (inner // OUT) + 3,)),
        ],
        compiler_params=ALL_VMEM,
    )(
        doc_lengths, block_order, layer_in, scan_in, out_grad, jnp.swapaxes(step_size, 1, 2),
        b_weight.T, c_weight.T, decay_rate[None],
    )
    cost = pl.CostEstimate(flops=10**9, bytes_accessed=10**6, transcendentals=0)
    got = exchange(send, SEQ)
    carried = pl.pallas_call(
        chain_kernel,
        out_shape=shape(blocks, 8, inner),
        in_specs=[SMEM, VMEM],
        out_specs=VMEM,
        scratch_shapes=[pltpu.SMEM((blocks,), jnp.int32)],
        compiler_params=PARAMS,
    )(block_order, got)
    back = exchange(carried, SEQ)
    came, keep, give = pl.pallas_call(
        grads_kernel,
        out_shape=(
            shape(state, inner, dtype=BF16),
            shape(state // 8 * tile_cols, 8, 128),
            shape(state // 8 * tile_cols, 8, 128),
        ),
        in_specs=[VMEM] * 7,
        out_specs=(VMEM,) * 3,
        scratch_shapes=[pltpu.VMEM((state, inner), BF16)],
        compiler_params=PARAMS,
        cost_estimate=cost,
    )(layer_in, back, pushed, seen, mats, scores, enter)
    given = swap_cores(give)
    scan_out = pl.pallas_call(
        output_kernel,
        out_shape=shape(1, rows, inner, dtype=BF16),
        in_specs=[VMEM] * 7,
        out_specs=VMEM,
        compiler_params=PARAMS,
        cost_estimate=cost,
    )(scan_in, skip_gain[None], came, pushed, scores, mats, enter)
    local = keep + given
    tiles = local.shape[0] // blocks
    share = jnp.sum(exchange(local.reshape(blocks, tiles, 8, 128), SEQ), axis=0)
    share = jnp.sum(everywhere(share, "z"), axis=0)
    mine = everywhere(share, SEQ).reshape(local.shape)
    other = swap_cores(mine)
    halves = (shape(state, width_in), shape(state, width_in))
    scratch = [pltpu.VMEM((state, width_in), F32), pltpu.SemaphoreType.DMA]
    partly = pl.pallas_call(
        place_mine_kernel,
        out_shape=halves,
        in_specs=[VMEM],
        out_specs=(HBM, HBM),
        scratch_shapes=scratch,
        compiler_params=PARAMS,
        cost_estimate=cost,
    )(mine)
    b_grad, c_grad = pl.pallas_call(
        place_other_kernel,
        out_shape=halves,
        in_specs=[VMEM, HBM, HBM],
        out_specs=(HBM, HBM),
        scratch_shapes=scratch,
        input_output_aliases={1: 0, 2: 1},
        compiler_params=PARAMS,
    )(other, *partly)
    return scan_out, b_grad.T, c_grad.T


def solution(mesh):
    seq = mesh.shape["seq"]
    side = 4 if seq % 4 == 0 else 1
    split = Mesh(
        mesh.devices.reshape(mesh.shape["dp"] // 2, 2, seq // side, side), ("z", "core", "y", "x")
    )
    rows = P(DP, SEQ, None)
    group = P(DP, None)
    in_specs = (rows, rows, rows, P(), P(), P(), P(), rows, group, group)
    return jax.shard_map(
        device_step, mesh=split, in_specs=in_specs, out_specs=(rows, P(), P()), check_vma=False
    )
```

```python
import jax
import jax.numpy as jnp
from jax import lax
from jax.experimental import pallas as pl
from jax.experimental.pallas import tpu as pltpu
from jax.sharding import Mesh
from jax.sharding import PartitionSpec as P


SEQ = ("y", "x")
DP = ("z", "core")
F32 = jnp.float32
BF16 = jnp.bfloat16
CHUNK = 256
EXTRA = 128
OUT = 512


VMEM = pl.BlockSpec(memory_space=pltpu.VMEM)
HBM = pl.BlockSpec(memory_space=pltpu.HBM)
SMEM = pl.BlockSpec(memory_space=pltpu.SMEM)
ALL_VMEM = pltpu.CompilerParams(vmem_limit_bytes=67043328)
PARAMS = pltpu.CompilerParams(vmem_limit_bytes=48 * 1024 * 1024)


def dot(a, b, dims=((1,), (0,))):
    return lax.dot_general(a, b, (dims, ((), ())), preferred_element_type=F32)


def dot_nt(a, b):
    return dot(a, b, ((1,), (1,)))


def dot_tn(a, b):
    return dot(a, b, ((0,), (0,)))


def slot_index():
    return lax.axis_index("y") * lax.axis_size("x") + lax.axis_index("x")


def spread(values, first, count, width):
    rows = max(values.shape[0], 8)
    table = jnp.broadcast_to(values, (rows, 128))
    lane = lax.broadcasted_iota(jnp.int32, (rows, 128), 1) // width
    per = 128 // width
    parts = [
        jnp.take_along_axis(table, lane + (first + j), axis=1, mode="promise_in_bounds")
        for j in range(0, count, per)
    ]
    whole = jnp.concatenate(parts, axis=1) if len(parts) > 1 else parts[0]
    return whole[: values.shape[0]]


def count_started(starts, position):
    return sum((start <= position).astype(jnp.int32) for start in starts)


def states_kernel(
    lengths_hbm, order_hbm, layer_hbm, x_hbm, grad_hbm, step_hbm, bw_hbm, cw_hbm, rate_hbm,
    send_hbm, pushed_hbm, seen_hbm, mats_hbm, scores_hbm, enter_hbm,
    lengths_ref, order_ref, layer_ref, x_ref, grad_ref, step_ref, weights_ref, rate_ref,
    send_ref, pushed_ref, seen_ref, mats_ref, scores_ref, enter_ref, in_sems, out_sems,
):
    state = bw_hbm.shape[0]
    pairs = (
        (lengths_hbm, lengths_ref), (order_hbm, order_ref), (rate_hbm, rate_ref),
        (step_hbm, step_ref), (layer_hbm, layer_ref), (bw_hbm, weights_ref.at[:state]),
        (cw_hbm, weights_ref.at[state:]),
        (x_hbm, x_ref), (grad_hbm, grad_ref),
    )
    copies = [pltpu.make_async_copy(a, b, in_sems.at[i]) for i, (a, b) in enumerate(pairs)]
    for copy in copies:
        copy.start()
    leaving = []

    def leave_for(from_ref, to_ref):
        copy = pltpu.make_async_copy(from_ref, to_ref, out_sems.at[len(leaving)])
        copy.start()
        leaving.append(copy)

    rows, inner = x_ref.shape[1:]
    heads = rate_ref.shape[1]
    width = inner // heads
    docs = lengths_ref.shape[1]
    blocks = send_ref.shape[0]
    half = blocks // 2
    for copy in copies[:4]:
        copy.wait()
    first = order_ref[0, slot_index()] * rows
    starts = [jnp.int32(0)]
    for j in range(docs - 1):
        starts.append(starts[-1] + lengths_ref[0, j])
    across = (rows, rows)
    at_row = lax.broadcasted_iota(jnp.int32, across, 0)
    at_column = lax.broadcasted_iota(jnp.int32, across, 1)
    column = count_started(starts, first + at_row)
    row = count_started(starts, first + at_column)
    before = count_started(starts, first - 1)
    last = count_started(starts, first + rows - 1)
    tri = at_row >= at_column
    causal = tri & (column == row)
    linked = column[:, :state] == before
    in_last = column[:, :state] == last
    logs_up = -(step_ref[0] * rate_ref[...].T)
    spare = jnp.zeros((128 - heads, rows), F32)
    cum = lax.dot_general(
        tri.astype(F32), jnp.concatenate([logs_up, spare], axis=0), (((1,), (1,)), ((), ())),
        precision=lax.Precision.HIGHEST, preferred_element_type=F32,
    )
    steps = jnp.concatenate([step_ref[0], spare], axis=0).T
    enter = jnp.exp(cum)
    leave = steps * jnp.exp(-cum)
    enter_ref[...] = enter
    whole = enter[rows - 1 :, :]
    total = whole * (before == last).astype(F32)
    send_ref[:, :, inner:] = jnp.broadcast_to(total[None], (blocks, 8, 128))
    for copy in copies[4:7]:
        copy.wait()
    mats = dot_nt(layer_ref[0], weights_ref[...]).astype(BF16)
    b_mat = mats[:, :state]
    c_mat = mats[:, state:]
    scores_ref[0] = jnp.where(causal, dot_nt(c_mat, b_mat), 0.0).astype(BF16)
    scores_ref[1] = causal.astype(F32).astype(BF16)
    b_last = jnp.where(in_last, b_mat.astype(F32), 0.0).astype(BF16)
    c_linked = jnp.where(linked, c_mat.astype(F32), 0.0).astype(BF16)
    mats_ref[0] = b_mat
    mats_ref[1] = c_mat
    mats_ref[2] = c_linked
    mats_ref[3] = linked.astype(F32).astype(BF16)
    mats_ref[4] = in_last.astype(F32).astype(BF16)
    for copy in copies[7:]:
        copy.wait()
    per = CHUNK // width
    for at in range(0, inner, CHUNK):
        cols = slice(at, at + CHUNK)
        h = at // width
        pushed = (spread(leave, h, per, width) * x_ref[0, :, cols].astype(F32)).astype(BF16)
        seen = (spread(enter, h, per, width) * grad_ref[0, :, cols].astype(F32)).astype(BF16)
        pushed_ref[:, cols] = pushed
        seen_ref[:, cols] = seen
        own = dot_tn(b_last, pushed) * spread(whole, h, per, width)
        adj = dot_tn(c_linked, seen)
        send_ref[:half, :, cols] = own.reshape(half, 8, CHUNK)
        send_ref[half:, :, cols] = adj.reshape(half, 8, CHUNK)
        if (at + CHUNK) % OUT == 0:
            done = slice(at + CHUNK - OUT, at + CHUNK)
            leave_for(pushed_ref.at[:, done], pushed_hbm.at[:, done])
            leave_for(seen_ref.at[:, done], seen_hbm.at[:, done])
            end = at + CHUNK + (128 if at + CHUNK == inner else 0)
            done = slice(at + CHUNK - OUT, end)
            leave_for(send_ref.at[:, :, done], send_hbm.at[:, :, done])
        if at == 0:
            leave_for(mats_ref, mats_hbm)
            leave_for(scores_ref, scores_hbm)
            leave_for(enter_ref, enter_hbm)
    for copy in leaving:
        copy.wait()


def chain_kernel(order_ref, got_ref, out_ref, held_ref, totals_ref):
    blocks, _, inner = out_ref.shape
    heads = inner // 64
    for slot in range(blocks):
        held_ref[order_ref[0, slot]] = jnp.int32(slot)
    backward = slot_index() >= blocks // 2
    totals = spread(got_ref[:, 0, inner:], 0, heads, 64)
    for slot in range(blocks):
        totals_ref[slot] = jnp.broadcast_to(totals[slot : slot + 1], (1, inner))
    carry = jnp.zeros(out_ref.shape[1:], F32)
    for k in range(blocks):
        slot = held_ref[jnp.where(backward, blocks - 1 - k, k)]
        out_ref[slot] = carry
        if k < blocks - 1:
            carry = carry * totals_ref[slot] + got_ref[slot, :, :inner]


def grads_kernel(
    layer_ref, got_ref, pushed_ref, seen_ref, mats_ref, scores_ref, enter_ref,
    came_ref, keep_ref, give_ref, ret_ref,
):
    rows, inner = pushed_ref.shape
    blocks = got_ref.shape[0]
    half = blocks // 2
    state = mats_ref.shape[2]
    whole = enter_ref[rows - 1 :, :]
    per = CHUNK // state
    for at in range(0, inner, CHUNK):
        cols = slice(at, at + CHUNK)
        back = got_ref[half:, :, cols].reshape(state, CHUNK)
        came_ref[:, cols] = got_ref[:half, :, cols].reshape(state, CHUNK).astype(BF16)
        ret_ref[:, cols] = (back * spread(whole, at // state, per, state)).astype(BF16)
    linked = mats_ref[3].astype(F32) > 0.5
    in_last = mats_ref[4].astype(F32) > 0.5
    pushed = pushed_ref[...]
    seen = seen_ref[...]
    causal = scores_ref[1].astype(F32) > 0.5
    mixing = jnp.where(causal, dot_nt(seen, pushed), 0.0).astype(BF16)
    d_b = dot_tn(mixing, mats_ref[1]) + jnp.where(in_last, dot_nt(pushed, ret_ref[...]), 0.0)
    d_c = dot(mixing, mats_ref[0]) + jnp.where(linked, dot_nt(seen, came_ref[...]), 0.0)
    scale = 1.0 / (rows * blocks * lax.axis_size("z") * lax.axis_size("core"))
    low = lax.axis_index("core") == 0
    mine = jnp.where(low, d_b, d_c).astype(BF16)
    other = jnp.where(low, d_c, d_b).astype(BF16)
    columns = layer_ref.shape[2] // 128
    for at in range(0, layer_ref.shape[2], CHUNK):
        tokens = layer_ref[0, :, at : at + CHUNK]
        for side, to_ref in ((other, give_ref), (mine, keep_ref)):
            part = dot_tn(side, tokens) * scale
            for r in range(state // 8):
                for c in range(CHUNK // 128):
                    tile = r * columns + at // 128 + c
                    to_ref[tile] = part[8 * r : 8 * r + 8, 128 * c : 128 * c + 128]


def output_kernel(x_ref, gain_ref, came_ref, pushed_ref, scores_ref, mats_ref, enter_ref, out_ref):
    inner = pushed_ref.shape[1]
    heads = gain_ref.shape[1]
    width = inner // heads
    scores = scores_ref[0]
    c_linked = mats_ref[2]
    enter = enter_ref[...]
    gain = jnp.concatenate([gain_ref[...].T, jnp.zeros((128 - heads, 1), F32)], axis=0).T
    per = CHUNK // width
    for at in range(0, inner, CHUNK):
        cols = slice(at, at + CHUNK)
        h = at // width
        mixed = dot(scores, pushed_ref[:, cols]) + dot(c_linked, came_ref[:, cols])
        skip = spread(gain, h, per, width) * x_ref[0, :, cols].astype(F32)
        out_ref[0, :, cols] = (spread(enter, h, per, width) * mixed + skip).astype(BF16)


def place(tiles_ref, whole_ref, b_hbm, c_hbm, to_b, sem):
    columns = whole_ref.shape[1] // 128
    for r in range(whole_ref.shape[0] // 8):
        for c in range(columns):
            whole_ref[8 * r : 8 * r + 8, 128 * c : 128 * c + 128] = tiles_ref[r * columns + c]

    @pl.when(to_b)
    def _():
        copy = pltpu.make_async_copy(whole_ref, b_hbm, sem)
        copy.start()
        copy.wait()

    @pl.when(jnp.logical_not(to_b))
    def _():
        copy = pltpu.make_async_copy(whole_ref, c_hbm, sem)
        copy.start()
        copy.wait()


def place_mine_kernel(tiles_ref, b_hbm, c_hbm, whole_ref, sem):
    place(tiles_ref, whole_ref, b_hbm, c_hbm, lax.axis_index("core") == 0, sem)


def place_other_kernel(tiles_ref, b_in, c_in, b_hbm, c_hbm, whole_ref, sem):
    place(tiles_ref, whole_ref, b_hbm, c_hbm, lax.axis_index("core") == 1, sem)


def shape(*dims, dtype=F32):
    return jax.ShapeDtypeStruct(dims, dtype)


def swap_cores(a):
    return lax.ppermute(a, "core", [(0, 1), (1, 0)])


def exchange(a, axes):
    return lax.all_to_all(a, axes, 0, 0, tiled=True)


def everywhere(a, axes):
    return exchange(jnp.broadcast_to(a[None], (lax.axis_size(axes),) + a.shape), axes)


def device_step(
    layer_in, scan_in, step_size, b_weight, c_weight, decay_rate, skip_gain, out_grad, doc_lengths,
    block_order,
):
    _, rows, inner = scan_in.shape
    width_in, state = b_weight.shape
    tile_cols = width_in // 128
    heads = decay_rate.shape[0]
    blocks = lax.axis_size(SEQ)
    docs = doc_lengths.shape[1]
    outs = (
        ((blocks, 8, inner + EXTRA), F32),
        ((rows, inner), BF16),
        ((rows, inner), BF16),
        ((5, rows, state), BF16),
        ((2, rows, rows), BF16),
        ((rows, 128), F32),
    )
    send, pushed, seen, mats, scores, enter = pl.pallas_call(
        states_kernel,
        out_shape=tuple(shape(*dims, dtype=dtype) for dims, dtype in outs),
        in_specs=[HBM] * 9,
        out_specs=(HBM,) * 6,
        scratch_shapes=[
            pltpu.SMEM((1, docs), jnp.int32),
            pltpu.SMEM((1, blocks), jnp.int32),
            pltpu.VMEM((1, rows, width_in), BF16),
            pltpu.VMEM((1, rows, inner), BF16),
            pltpu.VMEM((1, rows, inner), BF16),
            pltpu.VMEM((1, heads, rows), F32),
            pltpu.VMEM((2 * state, width_in), BF16),
            pltpu.VMEM((1, heads), F32),
            *[pltpu.VMEM(dims, dtype) for dims, dtype in outs],
            pltpu.SemaphoreType.DMA((9,)),
            pltpu.SemaphoreType.DMA((3 * (inner // OUT) + 3,)),
        ],
        compiler_params=ALL_VMEM,
    )(
        doc_lengths, block_order, layer_in, scan_in, out_grad, jnp.swapaxes(step_size, 1, 2),
        b_weight.T, c_weight.T, decay_rate[None],
    )
    cost = pl.CostEstimate(flops=10**9, bytes_accessed=10**6, transcendentals=0)
    got = exchange(send, SEQ)
    carried = pl.pallas_call(
        chain_kernel,
        out_shape=shape(blocks, 8, inner),
        in_specs=[SMEM, VMEM],
        out_specs=VMEM,
        scratch_shapes=[pltpu.SMEM((blocks,), jnp.int32), pltpu.VMEM((blocks, 1, inner), F32)],
        compiler_params=PARAMS,
    )(block_order, got)
    back = exchange(carried, SEQ)
    came, keep, give = pl.pallas_call(
        grads_kernel,
        out_shape=(
            shape(state, inner, dtype=BF16),
            shape(state // 8 * tile_cols, 8, 128),
            shape(state // 8 * tile_cols, 8, 128),
        ),
        in_specs=[VMEM] * 7,
        out_specs=(VMEM,) * 3,
        scratch_shapes=[pltpu.VMEM((state, inner), BF16)],
        compiler_params=PARAMS,
        cost_estimate=cost,
    )(layer_in, back, pushed, seen, mats, scores, enter)
    given = swap_cores(give)
    scan_out = pl.pallas_call(
        output_kernel,
        out_shape=shape(1, rows, inner, dtype=BF16),
        in_specs=[VMEM] * 7,
        out_specs=VMEM,
        compiler_params=PARAMS,
        cost_estimate=cost,
    )(scan_in, skip_gain[None], came, pushed, scores, mats, enter)
    local = keep + given
    tiles = local.shape[0] // blocks
    share = jnp.sum(exchange(local.reshape(blocks, tiles, 8, 128), SEQ), axis=0)
    share = jnp.sum(everywhere(share, "z"), axis=0)
    mine = everywhere(share, SEQ).reshape(local.shape)
    other = swap_cores(mine)
    halves = (shape(state, width_in), shape(state, width_in))
    scratch = [pltpu.VMEM((state, width_in), F32), pltpu.SemaphoreType.DMA]
    partly = pl.pallas_call(
        place_mine_kernel,
        out_shape=halves,
        in_specs=[VMEM],
        out_specs=(HBM, HBM),
        scratch_shapes=scratch,
        compiler_params=PARAMS,
        cost_estimate=cost,
    )(mine)
    b_grad, c_grad = pl.pallas_call(
        place_other_kernel,
        out_shape=halves,
        in_specs=[VMEM, HBM, HBM],
        out_specs=(HBM, HBM),
        scratch_shapes=scratch,
        input_output_aliases={1: 0, 2: 1},
        compiler_params=PARAMS,
    )(other, *partly)
    return scan_out, b_grad.T, c_grad.T


def solution(mesh):
    seq = mesh.shape["seq"]
    side = 4 if seq % 4 == 0 else 1
    split = Mesh(
        mesh.devices.reshape(mesh.shape["dp"] // 2, 2, seq // side, side), ("z", "core", "y", "x")
    )
    rows = P(DP, SEQ, None)
    group = P(DP, None)
    in_specs = (rows, rows, rows, P(), P(), P(), P(), rows, group, group)
    return jax.shard_map(
        device_step, mesh=split, in_specs=in_specs, out_specs=(rows, P(), P()), check_vma=False
    )
```

```python
import functools

import jax
import jax.numpy as jnp
from jax import lax
from jax.experimental import pallas as pl
from jax.experimental.pallas import tpu as pltpu
from jax.sharding import Mesh
from jax.sharding import PartitionSpec as P


SEQ = ("y", "x")
DP = ("z", "core")
F32 = jnp.float32
BF16 = jnp.bfloat16
CHUNK = 256
EXTRA = 128
OUT = 512


VMEM = pl.BlockSpec(memory_space=pltpu.VMEM)
HBM = pl.BlockSpec(memory_space=pltpu.HBM)
SMEM = pl.BlockSpec(memory_space=pltpu.SMEM)
ALL_VMEM = pltpu.CompilerParams(vmem_limit_bytes=67043328)
PARAMS = pltpu.CompilerParams(vmem_limit_bytes=48 * 1024 * 1024)


def dot(a, b, dims=((1,), (0,))):
    return lax.dot_general(a, b, (dims, ((), ())), preferred_element_type=F32)


def dot_nt(a, b):
    return dot(a, b, ((1,), (1,)))


def dot_tn(a, b):
    return dot(a, b, ((0,), (0,)))


def slot_index():
    return lax.axis_index("y") * lax.axis_size("x") + lax.axis_index("x")


def spread(values, first, count, width):
    rows = max(values.shape[0], 8)
    table = jnp.broadcast_to(values, (rows, 128))
    lane = lax.broadcasted_iota(jnp.int32, (rows, 128), 1) // width
    per = 128 // width
    parts = [
        jnp.take_along_axis(table, lane + (first + j), axis=1, mode="promise_in_bounds")
        for j in range(0, count, per)
    ]
    whole = jnp.concatenate(parts, axis=1) if len(parts) > 1 else parts[0]
    return whole[: values.shape[0]]


def count_started(starts, position):
    return sum((start <= position).astype(jnp.int32) for start in starts)


def states_kernel(
    lengths_hbm, order_hbm, layer_hbm, x_hbm, grad_hbm, step_hbm, bw_hbm, cw_hbm, rate_hbm,
    send_hbm, pushed_hbm, seen_hbm, mats_hbm, scores_hbm, enter_hbm,
    lengths_ref, order_ref, layer_ref, x_ref, grad_ref, step_ref, weights_ref, rate_ref,
    send_ref, pushed_ref, seen_ref, mats_ref, scores_ref, enter_ref, in_sems, out_sems,
):
    state = bw_hbm.shape[0]
    pairs = (
        (lengths_hbm, lengths_ref), (order_hbm, order_ref), (rate_hbm, rate_ref),
        (step_hbm, step_ref), (layer_hbm, layer_ref), (bw_hbm, weights_ref.at[:state]),
        (cw_hbm, weights_ref.at[state:]),
        (x_hbm, x_ref), (grad_hbm, grad_ref),
    )
    copies = [pltpu.make_async_copy(a, b, in_sems.at[i]) for i, (a, b) in enumerate(pairs)]
    for copy in copies:
        copy.start()
    leaving = []

    def leave_for(from_ref, to_ref):
        copy = pltpu.make_async_copy(from_ref, to_ref, out_sems.at[len(leaving)])
        copy.start()
        leaving.append(copy)

    rows, inner = x_ref.shape[1:]
    heads = rate_ref.shape[1]
    width = inner // heads
    docs = lengths_ref.shape[1]
    blocks = send_ref.shape[0]
    half = blocks // 2
    for copy in copies[:4]:
        copy.wait()
    first = order_ref[0, slot_index()] * rows
    starts = [jnp.int32(0)]
    for j in range(docs - 1):
        starts.append(starts[-1] + lengths_ref[0, j])
    across = (rows, rows)
    at_row = lax.broadcasted_iota(jnp.int32, across, 0)
    at_column = lax.broadcasted_iota(jnp.int32, across, 1)
    column = count_started(starts, first + at_row)
    row = count_started(starts, first + at_column)
    before = count_started(starts, first - 1)
    last = count_started(starts, first + rows - 1)
    tri = at_row >= at_column
    causal = tri & (column == row)
    linked = column[:, :state] == before
    in_last = column[:, :state] == last
    logs_up = -(step_ref[0] * rate_ref[...].T)
    spare = jnp.zeros((128 - heads, rows), F32)
    cum = lax.dot_general(
        tri.astype(F32), jnp.concatenate([logs_up, spare], axis=0), (((1,), (1,)), ((), ())),
        precision=lax.Precision.HIGHEST, preferred_element_type=F32,
    )
    steps = jnp.concatenate([step_ref[0], spare], axis=0).T
    enter = jnp.exp(cum)
    leave = steps * jnp.exp(-cum)
    enter_ref[...] = enter
    whole = enter[rows - 1 :, :]
    total = whole * (before == last).astype(F32)
    send_ref[:, :, inner:] = jnp.broadcast_to(total[None], (blocks, 8, 128))
    for copy in copies[4:7]:
        copy.wait()
    mats = dot_nt(layer_ref[0], weights_ref[...]).astype(BF16)
    b_mat = mats[:, :state]
    c_mat = mats[:, state:]
    scores_ref[0] = jnp.where(causal, dot_nt(c_mat, b_mat), 0.0).astype(BF16)
    scores_ref[1] = causal.astype(F32).astype(BF16)
    b_last = jnp.where(in_last, b_mat.astype(F32), 0.0).astype(BF16)
    c_linked = jnp.where(linked, c_mat.astype(F32), 0.0).astype(BF16)
    mats_ref[0] = b_mat
    mats_ref[1] = c_mat
    mats_ref[2] = c_linked
    mats_ref[3] = linked.astype(F32).astype(BF16)
    mats_ref[4] = in_last.astype(F32).astype(BF16)
    for copy in copies[7:]:
        copy.wait()
    per = CHUNK // width
    for at in range(0, inner, CHUNK):
        cols = slice(at, at + CHUNK)
        h = at // width
        pushed = (spread(leave, h, per, width) * x_ref[0, :, cols].astype(F32)).astype(BF16)
        seen = (spread(enter, h, per, width) * grad_ref[0, :, cols].astype(F32)).astype(BF16)
        pushed_ref[:, cols] = pushed
        seen_ref[:, cols] = seen
        own = dot_tn(b_last, pushed) * spread(whole, h, per, width)
        adj = dot_tn(c_linked, seen)
        send_ref[:half, :, cols] = own.reshape(half, 8, CHUNK)
        send_ref[half:, :, cols] = adj.reshape(half, 8, CHUNK)
        if (at + CHUNK) % OUT == 0:
            done = slice(at + CHUNK - OUT, at + CHUNK)
            leave_for(pushed_ref.at[:, done], pushed_hbm.at[:, done])
            leave_for(seen_ref.at[:, done], seen_hbm.at[:, done])
            end = at + CHUNK + (128 if at + CHUNK == inner else 0)
            done = slice(at + CHUNK - OUT, end)
            leave_for(send_ref.at[:, :, done], send_hbm.at[:, :, done])
        if at == 0:
            leave_for(mats_ref, mats_hbm)
            leave_for(scores_ref, scores_hbm)
            leave_for(enter_ref, enter_hbm)
    for copy in leaving:
        copy.wait()


def chain_kernel(order_ref, got_ref, out_ref, held_ref, totals_ref):
    blocks, _, inner = out_ref.shape
    heads = inner // 64
    for slot in range(blocks):
        held_ref[order_ref[0, slot]] = jnp.int32(slot)
    backward = slot_index() >= blocks // 2
    totals = spread(got_ref[:, 0, inner:], 0, heads, 64)
    for slot in range(blocks):
        totals_ref[slot] = jnp.broadcast_to(totals[slot : slot + 1], (1, inner))
    carry = jnp.zeros(out_ref.shape[1:], F32)
    for k in range(blocks):
        slot = held_ref[jnp.where(backward, blocks - 1 - k, k)]
        out_ref[slot] = carry
        if k < blocks - 1:
            carry = carry * totals_ref[slot] + got_ref[slot, :, :inner]


def grads_kernel(
    layer_ref, got_ref, pushed_ref, seen_ref, mats_ref, scores_ref, enter_ref,
    came_ref, mine_ref, give_ref, ret_ref,
):
    rows, inner = pushed_ref.shape
    blocks = got_ref.shape[0]
    half = blocks // 2
    state = mats_ref.shape[2]
    whole = enter_ref[rows - 1 :, :]
    per = CHUNK // state
    for at in range(0, inner, CHUNK):
        cols = slice(at, at + CHUNK)
        back = got_ref[half:, :, cols].reshape(state, CHUNK)
        came_ref[:, cols] = got_ref[:half, :, cols].reshape(state, CHUNK).astype(BF16)
        ret_ref[:, cols] = (back * spread(whole, at // state, per, state)).astype(BF16)
    linked = mats_ref[3].astype(F32) > 0.5
    in_last = mats_ref[4].astype(F32) > 0.5
    pushed = pushed_ref[...]
    seen = seen_ref[...]
    causal = scores_ref[1].astype(F32) > 0.5
    mixing = jnp.where(causal, dot_nt(seen, pushed), 0.0).astype(BF16)
    d_b = dot_tn(mixing, mats_ref[1]) + jnp.where(in_last, dot_nt(pushed, ret_ref[...]), 0.0)
    d_c = dot(mixing, mats_ref[0]) + jnp.where(linked, dot_nt(seen, came_ref[...]), 0.0)
    scale = 1.0 / (rows * blocks * lax.axis_size("z") * lax.axis_size("core"))
    low = lax.axis_index("core") == 0
    mine_ref[...] = jnp.where(low, d_b, d_c).astype(BF16)
    weight_tiles(jnp.where(low, d_c, d_b).astype(BF16), layer_ref, scale, give_ref)


def weight_tiles(side, layer_ref, scale, to_ref):
    columns = layer_ref.shape[2] // 128
    for at in range(0, layer_ref.shape[2], CHUNK):
        part = dot_tn(side, layer_ref[0, :, at : at + CHUNK]) * scale
        for r in range(side.shape[1] // 8):
            for c in range(CHUNK // 128):
                tile = r * columns + at // 128 + c
                to_ref[tile] = part[8 * r : 8 * r + 8, 128 * c : 128 * c + 128]


def keep_kernel(scale, layer_ref, mine_ref, keep_ref):
    weight_tiles(mine_ref[...], layer_ref, scale, keep_ref)


def output_kernel(x_ref, gain_ref, came_ref, pushed_ref, scores_ref, mats_ref, enter_ref, out_ref):
    inner = pushed_ref.shape[1]
    heads = gain_ref.shape[1]
    width = inner // heads
    scores = scores_ref[0]
    c_linked = mats_ref[2]
    enter = enter_ref[...]
    gain = jnp.concatenate([gain_ref[...].T, jnp.zeros((128 - heads, 1), F32)], axis=0).T
    per = CHUNK // width
    for at in range(0, inner, CHUNK):
        cols = slice(at, at + CHUNK)
        h = at // width
        mixed = dot(scores, pushed_ref[:, cols]) + dot(c_linked, came_ref[:, cols])
        skip = spread(gain, h, per, width) * x_ref[0, :, cols].astype(F32)
        out_ref[0, :, cols] = (spread(enter, h, per, width) * mixed + skip).astype(BF16)


def unpack_kernel(mine_ref, other_ref, b_ref, c_ref):
    columns = b_ref.shape[1] // 128

    def write(from_ref, to_ref):
        for r in range(to_ref.shape[0] // 8):
            for c in range(columns):
                to_ref[8 * r : 8 * r + 8, 128 * c : 128 * c + 128] = from_ref[r * columns + c]

    first = lax.axis_index("core") == 0

    @pl.when(first)
    def _():
        write(mine_ref, b_ref)
        write(other_ref, c_ref)

    @pl.when(jnp.logical_not(first))
    def _():
        write(other_ref, b_ref)
        write(mine_ref, c_ref)


def shape(*dims, dtype=F32):
    return jax.ShapeDtypeStruct(dims, dtype)


def swap_cores(a):
    return lax.ppermute(a, "core", [(0, 1), (1, 0)])


def exchange(a, axes):
    return lax.all_to_all(a, axes, 0, 0, tiled=True)


def everywhere(a, axes):
    return exchange(jnp.broadcast_to(a[None], (lax.axis_size(axes),) + a.shape), axes)


def device_step(
    layer_in, scan_in, step_size, b_weight, c_weight, decay_rate, skip_gain, out_grad, doc_lengths,
    block_order,
):
    _, rows, inner = scan_in.shape
    width_in, state = b_weight.shape
    tile_cols = width_in // 128
    heads = decay_rate.shape[0]
    blocks = lax.axis_size(SEQ)
    docs = doc_lengths.shape[1]
    outs = (
        ((blocks, 8, inner + EXTRA), F32),
        ((rows, inner), BF16),
        ((rows, inner), BF16),
        ((5, rows, state), BF16),
        ((2, rows, rows), BF16),
        ((rows, 128), F32),
    )
    send, pushed, seen, mats, scores, enter = pl.pallas_call(
        states_kernel,
        out_shape=tuple(shape(*dims, dtype=dtype) for dims, dtype in outs),
        in_specs=[HBM] * 9,
        out_specs=(HBM,) * 6,
        scratch_shapes=[
            pltpu.SMEM((1, docs), jnp.int32),
            pltpu.SMEM((1, blocks), jnp.int32),
            pltpu.VMEM((1, rows, width_in), BF16),
            pltpu.VMEM((1, rows, inner), BF16),
            pltpu.VMEM((1, rows, inner), BF16),
            pltpu.VMEM((1, heads, rows), F32),
            pltpu.VMEM((2 * state, width_in), BF16),
            pltpu.VMEM((1, heads), F32),
            *[pltpu.VMEM(dims, dtype) for dims, dtype in outs],
            pltpu.SemaphoreType.DMA((9,)),
            pltpu.SemaphoreType.DMA((3 * (inner // OUT) + 3,)),
        ],
        compiler_params=ALL_VMEM,
    )(
        doc_lengths, block_order, layer_in, scan_in, out_grad, jnp.swapaxes(step_size, 1, 2),
        b_weight.T, c_weight.T, decay_rate[None],
    )
    cost = pl.CostEstimate(flops=10**9, bytes_accessed=10**6, transcendentals=0)
    got = exchange(send, SEQ)
    carried = pl.pallas_call(
        chain_kernel,
        out_shape=shape(blocks, 8, inner),
        in_specs=[SMEM, VMEM],
        out_specs=VMEM,
        scratch_shapes=[pltpu.SMEM((blocks,), jnp.int32), pltpu.VMEM((blocks, 1, inner), F32)],
        compiler_params=PARAMS,
    )(block_order, got)
    back = exchange(carried, SEQ)
    came, own_side, give = pl.pallas_call(
        grads_kernel,
        out_shape=(
            shape(state, inner, dtype=BF16),
            shape(rows, state, dtype=BF16),
            shape(state // 8 * tile_cols, 8, 128),
        ),
        in_specs=[VMEM] * 7,
        out_specs=(VMEM,) * 3,
        scratch_shapes=[pltpu.VMEM((state, inner), BF16)],
        compiler_params=PARAMS,
        cost_estimate=cost,
    )(layer_in, back, pushed, seen, mats, scores, enter)
    given = swap_cores(give)
    keep = pl.pallas_call(
        functools.partial(keep_kernel, 1.0 / (rows * blocks * lax.axis_size(DP))),
        out_shape=shape(state // 8 * tile_cols, 8, 128),
        in_specs=[VMEM] * 2,
        out_specs=VMEM,
        compiler_params=PARAMS,
        cost_estimate=cost,
    )(layer_in, own_side)
    scan_out = pl.pallas_call(
        output_kernel,
        out_shape=shape(1, rows, inner, dtype=BF16),
        in_specs=[VMEM] * 7,
        out_specs=VMEM,
        compiler_params=PARAMS,
        cost_estimate=cost,
    )(scan_in, skip_gain[None], came, pushed, scores, mats, enter)
    local = keep + given
    tiles = local.shape[0] // blocks
    share = jnp.sum(exchange(local.reshape(blocks, tiles, 8, 128), SEQ), axis=0)
    share = jnp.sum(everywhere(share, "z"), axis=0)
    mine = everywhere(share, SEQ).reshape(local.shape)
    other = swap_cores(mine)
    b_grad, c_grad = pl.pallas_call(
        unpack_kernel,
        out_shape=(shape(state, width_in), shape(state, width_in)),
        in_specs=[VMEM] * 2,
        out_specs=(VMEM,) * 2,
        compiler_params=PARAMS,
    )(mine, other)
    return scan_out, b_grad.T, c_grad.T


def solution(mesh):
    seq = mesh.shape["seq"]
    side = 4 if seq % 4 == 0 else 1
    split = Mesh(
        mesh.devices.reshape(mesh.shape["dp"] // 2, 2, seq // side, side), ("z", "core", "y", "x")
    )
    rows = P(DP, SEQ, None)
    group = P(DP, None)
    in_specs = (rows, rows, rows, P(), P(), P(), P(), rows, group, group)
    return jax.shard_map(
        device_step, mesh=split, in_specs=in_specs, out_specs=(rows, P(), P()), check_vma=False
    )
```

```python
import functools

import jax
import jax.numpy as jnp
from jax import lax
from jax.experimental import pallas as pl
from jax.experimental.pallas import tpu as pltpu
from jax.sharding import Mesh
from jax.sharding import PartitionSpec as P


SEQ = ("y", "x")
DP = ("z", "core")
F32 = jnp.float32
BF16 = jnp.bfloat16
CHUNK = 256
EXTRA = 128
OUT = 512
PIECES = 2


VMEM = pl.BlockSpec(memory_space=pltpu.VMEM)
HBM = pl.BlockSpec(memory_space=pltpu.HBM)
SMEM = pl.BlockSpec(memory_space=pltpu.SMEM)
ALL_VMEM = pltpu.CompilerParams(vmem_limit_bytes=67043328)
PARAMS = pltpu.CompilerParams(vmem_limit_bytes=48 * 1024 * 1024)


def dot(a, b, dims=((1,), (0,))):
    return lax.dot_general(a, b, (dims, ((), ())), preferred_element_type=F32)


def dot_nt(a, b):
    return dot(a, b, ((1,), (1,)))


def dot_tn(a, b):
    return dot(a, b, ((0,), (0,)))


def slot_index():
    return lax.axis_index("y") * lax.axis_size("x") + lax.axis_index("x")


def spread(values, first, count, width):
    rows = max(values.shape[0], 8)
    table = jnp.broadcast_to(values, (rows, 128))
    lane = lax.broadcasted_iota(jnp.int32, (rows, 128), 1) // width
    per = 128 // width
    parts = [
        jnp.take_along_axis(table, lane + (first + j), axis=1, mode="promise_in_bounds")
        for j in range(0, count, per)
    ]
    whole = jnp.concatenate(parts, axis=1) if len(parts) > 1 else parts[0]
    return whole[: values.shape[0]]


def count_started(starts, position):
    return sum((start <= position).astype(jnp.int32) for start in starts)


def states_kernel(
    lengths_hbm, order_hbm, layer_hbm, x_hbm, grad_hbm, step_hbm, bw_hbm, cw_hbm, rate_hbm,
    send_hbm, pushed_hbm, seen_hbm, mats_hbm, scores_hbm, enter_hbm,
    lengths_ref, order_ref, layer_ref, x_ref, grad_ref, step_ref, weights_ref, rate_ref,
    send_ref, pushed_ref, seen_ref, mats_ref, scores_ref, enter_ref, in_sems, out_sems,
):
    state = bw_hbm.shape[0]
    pairs = (
        (lengths_hbm, lengths_ref), (order_hbm, order_ref), (rate_hbm, rate_ref),
        (step_hbm, step_ref), (layer_hbm, layer_ref), (bw_hbm, weights_ref.at[:state]),
        (cw_hbm, weights_ref.at[state:]),
        (x_hbm, x_ref), (grad_hbm, grad_ref),
    )
    copies = [pltpu.make_async_copy(a, b, in_sems.at[i]) for i, (a, b) in enumerate(pairs)]
    for copy in copies:
        copy.start()
    leaving = []

    def leave_for(from_ref, to_ref):
        copy = pltpu.make_async_copy(from_ref, to_ref, out_sems.at[len(leaving)])
        copy.start()
        leaving.append(copy)

    rows, inner = x_ref.shape[1:]
    heads = rate_ref.shape[1]
    width = inner // heads
    docs = lengths_ref.shape[1]
    blocks = send_ref.shape[0]
    half = blocks // 2
    for copy in copies[:4]:
        copy.wait()
    first = order_ref[0, slot_index()] * rows
    starts = [jnp.int32(0)]
    for j in range(docs - 1):
        starts.append(starts[-1] + lengths_ref[0, j])
    across = (rows, rows)
    at_row = lax.broadcasted_iota(jnp.int32, across, 0)
    at_column = lax.broadcasted_iota(jnp.int32, across, 1)
    column = count_started(starts, first + at_row)
    row = count_started(starts, first + at_column)
    before = count_started(starts, first - 1)
    last = count_started(starts, first + rows - 1)
    tri = at_row >= at_column
    causal = tri & (column == row)
    linked = column[:, :state] == before
    in_last = column[:, :state] == last
    logs_up = -(step_ref[0] * rate_ref[...].T)
    spare = jnp.zeros((128 - heads, rows), F32)
    cum = lax.dot_general(
        tri.astype(F32), jnp.concatenate([logs_up, spare], axis=0), (((1,), (1,)), ((), ())),
        precision=lax.Precision.HIGHEST, preferred_element_type=F32,
    )
    steps = jnp.concatenate([step_ref[0], spare], axis=0).T
    enter = jnp.exp(cum)
    leave = steps * jnp.exp(-cum)
    enter_ref[...] = enter
    whole = enter[rows - 1 :, :]
    total = whole * (before == last).astype(F32)
    send_ref[:, :, inner:] = jnp.broadcast_to(total[None], (blocks, 8, 128))
    for copy in copies[4:7]:
        copy.wait()
    mats = dot_nt(layer_ref[0], weights_ref[...]).astype(BF16)
    b_mat = mats[:, :state]
    c_mat = mats[:, state:]
    scores_ref[0] = jnp.where(causal, dot_nt(c_mat, b_mat), 0.0).astype(BF16)
    scores_ref[1] = causal.astype(F32).astype(BF16)
    b_last = jnp.where(in_last, b_mat.astype(F32), 0.0).astype(BF16)
    c_linked = jnp.where(linked, c_mat.astype(F32), 0.0).astype(BF16)
    mats_ref[0] = b_mat
    mats_ref[1] = c_mat
    mats_ref[2] = c_linked
    mats_ref[3] = linked.astype(F32).astype(BF16)
    mats_ref[4] = in_last.astype(F32).astype(BF16)
    for copy in copies[7:]:
        copy.wait()
    per = CHUNK // width
    for at in range(0, inner, CHUNK):
        cols = slice(at, at + CHUNK)
        h = at // width
        pushed = (spread(leave, h, per, width) * x_ref[0, :, cols].astype(F32)).astype(BF16)
        seen = (spread(enter, h, per, width) * grad_ref[0, :, cols].astype(F32)).astype(BF16)
        pushed_ref[:, cols] = pushed
        seen_ref[:, cols] = seen
        own = dot_tn(b_last, pushed) * spread(whole, h, per, width)
        adj = dot_tn(c_linked, seen)
        send_ref[:half, :, cols] = own.reshape(half, 8, CHUNK)
        send_ref[half:, :, cols] = adj.reshape(half, 8, CHUNK)
        if (at + CHUNK) % OUT == 0:
            done = slice(at + CHUNK - OUT, at + CHUNK)
            leave_for(pushed_ref.at[:, done], pushed_hbm.at[:, done])
            leave_for(seen_ref.at[:, done], seen_hbm.at[:, done])
            end = at + CHUNK + (128 if at + CHUNK == inner else 0)
            done = slice(at + CHUNK - OUT, end)
            leave_for(send_ref.at[:, :, done], send_hbm.at[:, :, done])
        if at == 0:
            leave_for(mats_ref, mats_hbm)
            leave_for(scores_ref, scores_hbm)
            leave_for(enter_ref, enter_hbm)
    for copy in leaving:
        copy.wait()


def chain_kernel(order_ref, got_ref, out_ref, held_ref, totals_ref):
    blocks, _, inner = out_ref.shape
    heads = inner // 64
    for slot in range(blocks):
        held_ref[order_ref[0, slot]] = jnp.int32(slot)
    backward = slot_index() >= blocks // 2
    totals = spread(got_ref[:, 0, inner:], 0, heads, 64)
    for slot in range(blocks):
        totals_ref[slot] = jnp.broadcast_to(totals[slot : slot + 1], (1, inner))
    carry = jnp.zeros(out_ref.shape[1:], F32)
    for k in range(blocks):
        slot = held_ref[jnp.where(backward, blocks - 1 - k, k)]
        out_ref[slot] = carry
        if k < blocks - 1:
            carry = carry * totals_ref[slot] + got_ref[slot, :, :inner]


def grads_kernel(
    layer_ref, got_ref, pushed_ref, seen_ref, mats_ref, scores_ref, enter_ref,
    came_ref, mine_ref, give_ref, ret_ref,
):
    rows, inner = pushed_ref.shape
    blocks = got_ref.shape[0]
    half = blocks // 2
    state = mats_ref.shape[2]
    whole = enter_ref[rows - 1 :, :]
    per = CHUNK // state
    for at in range(0, inner, CHUNK):
        cols = slice(at, at + CHUNK)
        back = got_ref[half:, :, cols].reshape(state, CHUNK)
        came_ref[:, cols] = got_ref[:half, :, cols].reshape(state, CHUNK).astype(BF16)
        ret_ref[:, cols] = (back * spread(whole, at // state, per, state)).astype(BF16)
    linked = mats_ref[3].astype(F32) > 0.5
    in_last = mats_ref[4].astype(F32) > 0.5
    pushed = pushed_ref[...]
    seen = seen_ref[...]
    causal = scores_ref[1].astype(F32) > 0.5
    mixing = jnp.where(causal, dot_nt(seen, pushed), 0.0).astype(BF16)
    d_b = dot_tn(mixing, mats_ref[1]) + jnp.where(in_last, dot_nt(pushed, ret_ref[...]), 0.0)
    d_c = dot(mixing, mats_ref[0]) + jnp.where(linked, dot_nt(seen, came_ref[...]), 0.0)
    scale = 1.0 / (rows * blocks * lax.axis_size("z") * lax.axis_size("core"))
    low = lax.axis_index("core") == 0
    mine_ref[...] = jnp.where(low, d_b, d_c).astype(BF16)
    weight_tiles(jnp.where(low, d_c, d_b).astype(BF16), layer_ref, scale, give_ref)


def weight_tiles(side, layer_ref, scale, to_ref):
    columns = layer_ref.shape[2] // 128
    for at in range(0, layer_ref.shape[2], CHUNK):
        part = dot_tn(side, layer_ref[0, :, at : at + CHUNK]) * scale
        for r in range(side.shape[1] // 8):
            for c in range(CHUNK // 128):
                tile = r * columns + at // 128 + c
                to_ref[tile] = part[8 * r : 8 * r + 8, 128 * c : 128 * c + 128]


def keep_kernel(scale, layer_ref, mine_ref, keep_ref):
    weight_tiles(mine_ref[...], layer_ref, scale, keep_ref)


def output_kernel(x_ref, gain_ref, came_ref, pushed_ref, scores_ref, mats_ref, enter_ref, out_ref):
    inner = pushed_ref.shape[1]
    heads = gain_ref.shape[1]
    width = inner // heads
    scores = scores_ref[0]
    c_linked = mats_ref[2]
    enter = enter_ref[...]
    gain = jnp.concatenate([gain_ref[...].T, jnp.zeros((128 - heads, 1), F32)], axis=0).T
    per = CHUNK // width
    for at in range(0, inner, CHUNK):
        cols = slice(at, at + CHUNK)
        h = at // width
        mixed = dot(scores, pushed_ref[:, cols]) + dot(c_linked, came_ref[:, cols])
        skip = spread(gain, h, per, width) * x_ref[0, :, cols].astype(F32)
        out_ref[0, :, cols] = (spread(enter, h, per, width) * mixed + skip).astype(BF16)


def unpack_kernel(mine_ref, other_ref, b_hbm, c_hbm, mine_whole, other_whole, sems):
    state, width = mine_whole.shape
    columns = width // 128
    piece = state // PIECES
    low = lax.axis_index("core") == 0
    to_low, to_high = [], []
    for side, (from_ref, whole) in enumerate(((mine_ref, mine_whole), (other_ref, other_whole))):
        for p in range(PIECES):
            for r in range(p * piece // 8, (p + 1) * piece // 8):
                for c in range(columns):
                    whole[8 * r : 8 * r + 8, 128 * c : 128 * c + 128] = from_ref[r * columns + c]
            rows = slice(p * piece, (p + 1) * piece)
            sem = sems.at[side * PIECES + p]
            ends = (b_hbm, c_hbm) if side == 0 else (c_hbm, b_hbm)
            first = pltpu.make_async_copy(whole.at[rows], ends[0].at[rows], sem)
            second = pltpu.make_async_copy(whole.at[rows], ends[1].at[rows], sem)
            pl.when(low)(first.start)
            pl.when(jnp.logical_not(low))(second.start)
            to_low.append(first)
            to_high.append(second)

    @pl.when(low)
    def _():
        for copy in to_low:
            copy.wait()

    @pl.when(jnp.logical_not(low))
    def _():
        for copy in to_high:
            copy.wait()


def shape(*dims, dtype=F32):
    return jax.ShapeDtypeStruct(dims, dtype)


def swap_cores(a):
    return lax.ppermute(a, "core", [(0, 1), (1, 0)])


def exchange(a, axes):
    return lax.all_to_all(a, axes, 0, 0, tiled=True)


def everywhere(a, axes):
    return exchange(jnp.broadcast_to(a[None], (lax.axis_size(axes),) + a.shape), axes)


def device_step(
    layer_in, scan_in, step_size, b_weight, c_weight, decay_rate, skip_gain, out_grad, doc_lengths,
    block_order,
):
    _, rows, inner = scan_in.shape
    width_in, state = b_weight.shape
    tile_cols = width_in // 128
    heads = decay_rate.shape[0]
    blocks = lax.axis_size(SEQ)
    docs = doc_lengths.shape[1]
    outs = (
        ((blocks, 8, inner + EXTRA), F32),
        ((rows, inner), BF16),
        ((rows, inner), BF16),
        ((5, rows, state), BF16),
        ((2, rows, rows), BF16),
        ((rows, 128), F32),
    )
    send, pushed, seen, mats, scores, enter = pl.pallas_call(
        states_kernel,
        out_shape=tuple(shape(*dims, dtype=dtype) for dims, dtype in outs),
        in_specs=[HBM] * 9,
        out_specs=(HBM,) * 6,
        scratch_shapes=[
            pltpu.SMEM((1, docs), jnp.int32),
            pltpu.SMEM((1, blocks), jnp.int32),
            pltpu.VMEM((1, rows, width_in), BF16),
            pltpu.VMEM((1, rows, inner), BF16),
            pltpu.VMEM((1, rows, inner), BF16),
            pltpu.VMEM((1, heads, rows), F32),
            pltpu.VMEM((2 * state, width_in), BF16),
            pltpu.VMEM((1, heads), F32),
            *[pltpu.VMEM(dims, dtype) for dims, dtype in outs],
            pltpu.SemaphoreType.DMA((9,)),
            pltpu.SemaphoreType.DMA((3 * (inner // OUT) + 3,)),
        ],
        compiler_params=ALL_VMEM,
    )(
        doc_lengths, block_order, layer_in, scan_in, out_grad, jnp.swapaxes(step_size, 1, 2),
        b_weight.T, c_weight.T, decay_rate[None],
    )
    cost = pl.CostEstimate(flops=10**9, bytes_accessed=10**6, transcendentals=0)
    got = exchange(send, SEQ)
    carried = pl.pallas_call(
        chain_kernel,
        out_shape=shape(blocks, 8, inner),
        in_specs=[SMEM, VMEM],
        out_specs=VMEM,
        scratch_shapes=[pltpu.SMEM((blocks,), jnp.int32), pltpu.VMEM((blocks, 1, inner), F32)],
        compiler_params=PARAMS,
    )(block_order, got)
    back = exchange(carried, SEQ)
    came, own_side, give = pl.pallas_call(
        grads_kernel,
        out_shape=(
            shape(state, inner, dtype=BF16),
            shape(rows, state, dtype=BF16),
            shape(state // 8 * tile_cols, 8, 128),
        ),
        in_specs=[VMEM] * 7,
        out_specs=(VMEM,) * 3,
        scratch_shapes=[pltpu.VMEM((state, inner), BF16)],
        compiler_params=PARAMS,
        cost_estimate=cost,
    )(layer_in, back, pushed, seen, mats, scores, enter)
    given = swap_cores(give)
    keep = pl.pallas_call(
        functools.partial(keep_kernel, 1.0 / (rows * blocks * lax.axis_size(DP))),
        out_shape=shape(state // 8 * tile_cols, 8, 128),
        in_specs=[VMEM] * 2,
        out_specs=VMEM,
        compiler_params=PARAMS,
        cost_estimate=cost,
    )(layer_in, own_side)
    scan_out = pl.pallas_call(
        output_kernel,
        out_shape=shape(1, rows, inner, dtype=BF16),
        in_specs=[VMEM] * 7,
        out_specs=VMEM,
        compiler_params=PARAMS,
        cost_estimate=cost,
    )(scan_in, skip_gain[None], came, pushed, scores, mats, enter)
    local = keep + given
    tiles = local.shape[0] // blocks
    share = jnp.sum(exchange(local.reshape(blocks, tiles, 8, 128), SEQ), axis=0)
    share = jnp.sum(everywhere(share, "z"), axis=0)
    mine = everywhere(share, SEQ).reshape(local.shape)
    other = swap_cores(mine)
    b_grad, c_grad = pl.pallas_call(
        unpack_kernel,
        out_shape=(shape(state, width_in), shape(state, width_in)),
        in_specs=[VMEM] * 2,
        out_specs=(HBM,) * 2,
        scratch_shapes=[
            pltpu.VMEM((state, width_in), F32),
            pltpu.VMEM((state, width_in), F32),
            pltpu.SemaphoreType.DMA((2 * PIECES,)),
        ],
        compiler_params=PARAMS,
    )(mine, other)
    return scan_out, b_grad.T, c_grad.T


def solution(mesh):
    seq = mesh.shape["seq"]
    side = 4 if seq % 4 == 0 else 1
    split = Mesh(
        mesh.devices.reshape(mesh.shape["dp"] // 2, 2, seq // side, side), ("z", "core", "y", "x")
    )
    rows = P(DP, SEQ, None)
    group = P(DP, None)
    in_specs = (rows, rows, rows, P(), P(), P(), P(), rows, group, group)
    return jax.shard_map(
        device_step, mesh=split, in_specs=in_specs, out_specs=(rows, P(), P()), check_vma=False
    )
```
